256 devices in a mesh: dp: 8 (over z_lo, core), fsdp: 32 (over y, x, z_hi).
Axes of the slice: x: 4, y: 4, z: 8 (z_hi: 2, z_lo: 4; z = z_hi * 4 + z_lo), core: 2. Of those that a mesh axis runs over, the one named last changes fastest.
Arguments:
- hidden_states: bfloat16 [1024, 4096], P(('dp', 'fsdp')), may hold values from -400 to 400
- token_ids: int32 [1024], P(('dp', 'fsdp')), may hold values from 0 to 4095
- norm_gain: float32 [4096], replicated, may hold values from 0.5 to 1.5
- ref_gate_w: bfloat16 [4096, 14784], P('dp', 'fsdp'), may hold values from -0.1875 to 0.1875
- ref_up_w: bfloat16 [4096, 14784], P('dp', 'fsdp'), may hold values from -0.1875 to 0.1875
- ref_down_w: bfloat16 [14784, 4096], P('fsdp', 'dp'), may hold values from -0.09375 to 0.09375
- pol_gate_w: bfloat16 [4096, 14784], P('dp', 'fsdp'), may hold values from -0.1875 to 0.1875
- pol_up_w: bfloat16 [4096, 14784], P('dp', 'fsdp'), may hold values from -0.1875 to 0.1875
- pol_down_w: bfloat16 [14784, 4096], P('fsdp', 'dp'), may hold values from -0.09375 to 0.09375
- sample_lengths: int32 [8, 32], P('dp'), may hold values from 1 to 24, 128 in all within a row
- prompt_index: int32 [8, 32], P('dp'), may hold values from 0 to 3, as said below
- rewards: float32 [8, 32], P('dp'), may hold values from -6 to 6
Outputs:
- grad_gate: float32 [4096, 14784], P('dp', 'fsdp')
- grad_up: float32 [4096, 14784], P('dp', 'fsdp')
- grad_down: float32 [14784, 4096], P('fsdp', 'dp')
- advantage: float32 [8, 32], P('dp')
The draws below stay inside these ranges and needn't reach their ends.
Inputs may be any that keep to these rules, and one draw needn't show every extreme that they name: `prompt_index`: in each row, every prompt from 0 to 3 is answered by exactly 8 samples. `sample_lengths`: each row sums to 128.
All inputs are finite; a program needn't handle non-finite values.
Results may differ from the reference program's by a relative error of at most 0.013.
Values may be sent and summed in bfloat16 or wider, within the bound.
A program may use at most 64 MiB of HBM per device.

```python
import math
import jax
import jax.numpy as jnp
import numpy as np
from jax import lax

D = 4096
FF = 14784
K = 8
SAMPLES_G = 32
GROUP_TOK = 128
MOST_LEN = 24
TOKENS = 1024
N_DP = 8


def one_order(single_key):
    return jax.random.permutation(single_key, SAMPLES_G)


def draw_prompt_index(key, part):
    row_keys = jax.random.split(jax.random.fold_in(key, 17), N_DP)
    orders = jax.vmap(one_order)(row_keys)
    return (orders // K).astype(jnp.int32)


def draw_hidden_states(key, part):
    first = jax.random.fold_in(jax.random.fold_in(key, 29), 0)
    values = 0.5 * jnp.clip(jax.random.normal(first, (TOKENS, D), jnp.float32), -5.0, 5.0)
    return values.astype(jnp.bfloat16)


def place_ends(values, rng, least, top_value):
    spot = [jax.random.randint(jax.random.fold_in(rng, axis), (), 0, length) for axis, length in enumerate(values.shape)]
    main_axis = values.shape.index(max(values.shape))
    neighbour = spot[:main_axis] + [(spot[main_axis] + 1) % values.shape[main_axis]] + spot[main_axis + 1:]
    return values.at[tuple(spot)].set(least).at[tuple(neighbour)].set(top_value)


def block_levels(rng, dims, pieces, low, high):
    def one(dim, shards_of):
        steps = jax.random.uniform(jax.random.fold_in(jax.random.fold_in(rng, 6), dim), (shards_of,), jnp.float32, low / len(pieces), high / len(pieces))
        return jnp.repeat(jnp.exp(steps), dims[dim] // shards_of).reshape((-1,) + (1,) * (len(dims) - dim - 1))

    gain = one(*pieces[0])
    for cut in pieces[1:]:
        gain = gain * one(*cut)
    return gain


def length_profile(number_of, total, limit, slope):
    loads = [(1 << 20) // math.isqrt(standing ** slope) + 1 for standing in range(2, number_of + 1)]
    rest, holding = total - limit - (number_of - 1), [1] * (number_of - 1)
    while rest > 0:
        free = [i for i in range(number_of - 1) if holding[i] < limit]
        pool, budget = sum([loads[i] for i in free]), rest
        for i in free:
            more = min(limit - holding[i], max(1, budget * loads[i] // pool), rest)
            holding[i] = holding[i] + more
            rest = rest - more
    return np.array([limit] + holding)


def ragged(own_key, number_of, total, limit, lean):
    if number_of == 2:
        one = jax.random.randint(own_key, (), max(1, total - limit), min(limit, total - 1) + 1)
        return jnp.stack([one, total - one])
    tallies = jnp.asarray(length_profile(number_of, total, limit, lean), jnp.int32)
    pairs = (number_of - 1) // 2
    source_of, receiver = tallies[1:1 + 2 * pairs:2], tallies[2:2 + 2 * pairs:2]
    slack = jnp.minimum(source_of - 1, limit - receiver)
    passed = jax.random.randint(jax.random.fold_in(own_key, 1), (pairs,), 0, 1 << 20) % (slack + 1)
    tallies = tallies.at[1:1 + 2 * pairs:2].set(source_of - passed).at[2:2 + 2 * pairs:2].set(receiver + passed)
    return tallies[jax.random.permutation(jax.random.fold_in(own_key, 2), number_of)]


def noise(own_key, shape, spread, reach, pieces=(), held_as=jnp.bfloat16):
    gain = block_levels(own_key, shape, pieces, -0.22, 0.18) if pieces else 1.0
    values = jax.random.normal(own_key, shape, jnp.float32) * spread * gain
    return jnp.minimum(jnp.maximum(values, -reach), reach).astype(held_as)


def setup_inputs(seed: int = 0) -> dict:
    key_list = jax.random.split(jax.random.key(seed), 13)
    return {
        "hidden_states": draw_hidden_states(jax.random.fold_in(key_list[12], 71), 0),
        "token_ids": place_ends(jax.random.randint(key_list[1], (TOKENS,), 0, D), jax.random.fold_in(key_list[1], 1), 0, D - 1).astype(jnp.int32),
        "norm_gain": jnp.clip(1.0 + 0.1 * jax.random.normal(key_list[2], (D,), jnp.float32), 0.5, 1.5),
        "ref_gate_w": noise(key_list[3], (D, FF), (D // 4) ** -0.5, 0.1875, ((0, 8), (1, 32))),
        "ref_up_w": noise(key_list[4], (D, FF), (D // 4) ** -0.5, 0.1875, ((0, 8), (1, 32))),
        "ref_down_w": noise(key_list[5], (FF, D), (FF // 4) ** -0.5, 0.09375, ((0, 32), (1, 8))),
        "pol_gate_w": noise(key_list[6], (D, FF), (D // 4) ** -0.5, 0.1875, ((0, 8), (1, 32))),
        "pol_up_w": noise(key_list[7], (D, FF), (D // 4) ** -0.5, 0.1875, ((0, 8), (1, 32))),
        "pol_down_w": noise(key_list[8], (FF, D), (FF // 4) ** -0.5, 0.09375, ((0, 32), (1, 8))),
        "sample_lengths": jax.vmap(lambda own: ragged(own, SAMPLES_G, GROUP_TOK, MOST_LEN, 1))(jax.random.split(key_list[9], N_DP)).reshape((N_DP, SAMPLES_G)).astype(jnp.int32),
        "prompt_index": draw_prompt_index(jax.random.fold_in(key_list[12], 71), 0),
        "rewards": noise(key_list[11], (N_DP, SAMPLES_G), 1.0, 6.0, ((0, 8),), jnp.float32),
    }


EPSILON = 1e-06
KL_WEIGHT = 0.05

def normalize(states, norm_gain):
    values = states.astype(jnp.float32)
    factor = lax.rsqrt(lax.optimization_barrier(jnp.mean(values * values, axis=-1, keepdims=True)) + EPSILON)
    return (values * factor * norm_gain).astype(jnp.bfloat16)

def block_forward(normed, gate_w, up_w, down_w):
    gate_pre = jnp.dot(normed, gate_w, preferred_element_type=jnp.float32)
    up_pre = jnp.dot(normed, up_w, preferred_element_type=jnp.float32)
    hidden = (jax.nn.silu(gate_pre) * up_pre).astype(jnp.bfloat16)
    output = jnp.dot(hidden, down_w, preferred_element_type=jnp.float32)
    return (gate_pre, up_pre, hidden, output)

def token_logprob(logits, token_ids):
    row_peak = lax.optimization_barrier(jnp.max(logits, axis=-1))
    log_total = row_peak + jnp.log(lax.optimization_barrier(jnp.sum(jnp.exp(logits - row_peak[:, None]), axis=-1)))
    columns = jnp.arange(logits.shape[1], dtype=jnp.int32)
    picked = lax.optimization_barrier(jnp.sum(jnp.where(columns[None, :] == token_ids[:, None], logits, 0.0), axis=-1))
    return (picked - log_total, log_total)

def grouped_product(left_rows, right_rows, groups):
    left_groups = left_rows.reshape(groups, -1, left_rows.shape[1])
    right_groups = right_rows.reshape(groups, -1, right_rows.shape[1])

    def accumulate(running, couple):
        product = jnp.dot(couple[0].T, couple[1], preferred_element_type=jnp.float32)
        rounded = lax.optimization_barrier(product.astype(jnp.bfloat16))
        return (running + rounded.astype(jnp.float32), None)
    start_sum = jnp.zeros((left_rows.shape[1], right_rows.shape[1]), jnp.float32)
    result, _ = lax.scan(accumulate, start_sum, (left_groups, right_groups))
    return result

def reference(hidden_states, token_ids, norm_gain, ref_gate_w, ref_up_w, ref_down_w, pol_gate_w, pol_up_w, pol_down_w, sample_lengths, prompt_index, rewards):
    normed = normalize(hidden_states, norm_gain)
    states = hidden_states.astype(jnp.float32)
    _, _, _, ref_out = block_forward(normed, ref_gate_w, ref_up_w, ref_down_w)
    ref_lp, _ = token_logprob(states + ref_out, token_ids)
    gate_pre, up_pre, hidden, pol_out = block_forward(normed, pol_gate_w, pol_up_w, pol_down_w)
    logits = states + pol_out
    pol_lp, log_total = token_logprob(logits, token_ids)
    groups = sample_lengths.shape[0]
    group_tokens = hidden_states.shape[0] // groups
    sample_ends = jnp.cumsum(sample_lengths, axis=-1)
    sample_starts = sample_ends - sample_lengths
    position = jnp.arange(group_tokens, dtype=jnp.int32)
    inside = ((position[None, :, None] >= sample_starts[:, None, :]) & (position[None, :, None] < sample_ends[:, None, :])).astype(jnp.float32)
    log_gap = (pol_lp - ref_lp).reshape(groups, group_tokens)
    divergence = jnp.einsum('gt,gts->gs', log_gap, inside)
    scores = rewards - KL_WEIGHT * divergence
    same_prompt = (prompt_index[:, :, None] == prompt_index[:, None, :]).astype(jnp.float32)
    others = jnp.einsum('gst,gt->gs', same_prompt, scores) - scores
    advantage = scores - others / (K - 1)
    weight = jnp.einsum('gts,gs->gt', inside, advantage).reshape(-1)
    columns = jnp.arange(logits.shape[1], dtype=jnp.int32)
    onehot = (columns[None, :] == token_ids[:, None]).astype(jnp.float32)
    grad_logits = (-weight[:, None] * (onehot - jnp.exp(logits - log_total[:, None]))).astype(jnp.bfloat16)
    grad_hidden = lax.dot_general(grad_logits, pol_down_w, (((1,), (1,)), ((), ())), preferred_element_type=jnp.float32)
    sigmoid_gate = jax.nn.sigmoid(gate_pre)
    grad_gate_pre = (grad_hidden * up_pre * sigmoid_gate * (1.0 + gate_pre * (1.0 - sigmoid_gate))).astype(jnp.bfloat16)
    grad_up_pre = (grad_hidden * gate_pre * sigmoid_gate).astype(jnp.bfloat16)
    grad_down = grouped_product(hidden, grad_logits, groups)
    grad_inner = grouped_product(normed, jnp.concatenate([grad_gate_pre, grad_up_pre], axis=1), groups)
    unit_count = gate_pre.shape[1]
    return (grad_inner[:, :unit_count], grad_inner[:, unit_count:], grad_down, advantage)
```

```python
import functools
from types import SimpleNamespace

import jax
import jax.numpy as jnp
from jax import lax
from jax.experimental import pallas as pl
from jax.experimental.pallas import tpu as pltpu
from jax.sharding import PartitionSpec as P

K = 8
EPSILON = 1e-06
KL_WEIGHT = 0.05

F32 = jnp.float32
BF16 = jnp.bfloat16
DMA = pltpu.SemaphoreType.DMA
VMEM = pl.BlockSpec(memory_space=pltpu.VMEM)

LANES = 128
PLANE = 16
CHIPS = 4
SKEW = 2


def copy_to(src, dst, send, recv, **where):
    return pltpu.make_async_remote_copy(
        src_ref=src,
        dst_ref=dst,
        send_sem=send,
        recv_sem=recv,
        device_id=where,
        device_id_type=pl.DeviceIdType.MESH,
    )


def signal(**where):
    pl.semaphore_signal(
        pltpu.get_barrier_semaphore(),
        inc=1,
        device_id=where,
        device_id_type=pl.DeviceIdType.MESH,
    )


def each(start, stop, body):
    def step(index, carry):
        body(index)
        return carry

    lax.fori_loop(start, stop, step, 0)


def greet_all(me, groups, member):
    plane, half = member // 2, member % 2
    mate = member + 1 - 2 * half

    def row(step):
        signal(dp=lax.rem(me + step, groups))

    def flat(step):
        signal(fsdp=lax.rem(plane + step, PLANE) * 2 + half)

    each(1, groups, row)
    each(1, PLANE, flat)
    signal(fsdp=mate)
    pl.semaphore_wait(pltpu.get_barrier_semaphore(), groups - 1 + PLANE - 1 + 1)


def row_exchange(me, groups, sent, landed, send, recv):
    def copy(step):
        peer = lax.rem(me + step, groups)
        return copy_to(sent(peer), landed(me), send.at[step], recv.at[me], dp=peer)

    def wait(step):
        source = lax.rem(me + groups - step, groups)
        copy_to(sent(source), landed(source), send.at[step], recv.at[source], dp=source).wait_recv()

    return (
        lambda: each(1, groups, lambda step: copy(step).start()),
        lambda: each(1, groups, wait),
        lambda: each(1, groups, lambda step: copy(step).wait_send()),
    )


def plane_gather(member, views, mate_send, mate_recv, send, recv, meanwhile=lambda: None):
    plane, half = member // 2, member % 2
    mate = member + 1 - 2 * half

    def mate_copy(i, block):
        view = views[i](block)
        return copy_to(view, view, mate_send.at[i], mate_recv.at[i], fsdp=mate)

    def flat(i, which, block, step):
        view = views[i](block)
        peer = lax.rem(plane + step, PLANE) * 2 + half
        return copy_to(
            view, view, send.at[i, which, step], recv.at[i, which, plane], fsdp=peer
        )

    def flat_wait(i, which, step):
        source = lax.rem(plane + PLANE - step, PLANE)
        view = views[i](source * 2 + (half if which == 0 else 1 - half))
        copy_to(
            view, view, send.at[i, which, step], recv.at[i, which, source], fsdp=source * 2 + half
        ).wait_recv()

    count = range(len(views))
    for i in count:
        mate_copy(i, member).start()
    each(1, PLANE, lambda step: [flat(i, 0, member, step).start() for i in count])
    meanwhile()
    for i in count:
        mate_copy(i, mate).wait_recv()
    each(1, PLANE, lambda step: [flat(i, 1, mate, step).start() for i in count])
    each(1, PLANE, lambda step: [flat_wait(i, 0, step) for i in count])
    each(1, PLANE, lambda step: [flat_wait(i, 1, step) for i in count])
    for i in count:
        mate_copy(i, member).wait_send()
    each(1, PLANE, lambda step: [flat(i, 0, member, step).wait_send() for i in count])
    each(1, PLANE, lambda step: [flat(i, 1, mate, step).wait_send() for i in count])


def norm_phase(s, groups, me, member):
    count, width = s.rows.shape
    block = width // groups
    values = s.rows[...].astype(F32)
    factor = lax.rsqrt(jnp.mean(values * values, axis=-1, keepdims=True) + EPSILON)
    for d in range(groups):
        s.row_sent[d] = s.rows[:, d * block : (d + 1) * block]
    s.meta_sent[...] = jnp.zeros_like(s.meta_sent)
    small = (s.lengths, s.prompts, s.rewards, s.ids)
    for i, value in enumerate(small):
        s.meta_sent[i : i + 1, 0 : value.shape[1]] = value[...].astype(F32)
    s.meta_sent[4 : 4 + count, :] = jnp.broadcast_to(factor, (count, LANES))
    moves = (
        row_exchange(
            me, groups, lambda p: s.row_sent.at[p], lambda g: s.row_landed.at[g], s.r_send, s.r_recv
        ),
        row_exchange(
            me, groups, lambda p: s.meta_sent, lambda g: s.meta.at[g], s.m_send, s.m_recv
        ),
    )
    for start, _, _ in moves:
        start()
    s.row_landed[me] = s.row_sent[me]
    s.meta[me] = s.meta_sent[...]
    for _, wait, _ in moves:
        wait()
    gain = s.gain[:, pl.ds(pl.multiple_of(me * block, block), block)]
    for g in range(groups):
        state = s.row_landed[g].astype(F32)
        s.states[g * count : (g + 1) * count, :] = state
        s.scaled[g * count : (g + 1) * count, :] = state * s.meta[g, 4 : 4 + count, 0:1] * gain
    rows = groups * count
    view = lambda b: s.normed.at[pl.ds(pl.multiple_of(b * rows, rows), rows), :]
    s.normed[pl.ds(pl.multiple_of(member * rows, rows), rows), :] = s.scaled[...].astype(BF16)

    def columns_of_ids():
        ids = turned([s.meta[g, 3:4, :] for g in range(groups)])
        for g in range(groups):
            s.id_rows[g * count : (g + 1) * count, :] = jnp.broadcast_to(
                ids[0:count, g : g + 1], (count, LANES)
            )

    plane_gather(
        member, (view,), s.n_mate_send, s.n_mate_recv, s.n_send, s.n_recv, columns_of_ids
    )
    for _, _, finish in moves:
        finish()


def run_reduce(steps, skew, me, plane, product, finish, gathered, s, arrived=None):
    chip, core = me // 2, me % 2
    partner = me + 1 - 2 * core
    quarter = s.own.shape[2]
    block = quarter // 4
    chunk = quarter // steps
    per = steps // 4
    lows = s.sent.shape[1] if s.sent is not None else 0
    count = s.own.shape[1]
    pairs = [(s.sent, s.landed, s.pair_send, s.pair_recv)]
    if s.high_sent is not None:
        pairs.append((s.high_sent, s.high_landed, s.high_send, s.high_recv))

    def pair_copies(e):
        return [
            copy_to(a.at[e], b.at[e], send.at[e], recv.at[e], dp=partner)
            for a, b, send, recv in pairs
        ]

    def place(e, c, b):
        return lax.rem(plane + 1 + 4 * b + 2 * e + c, PLANE)

    def left_rows(ref, e, c):
        return jnp.concatenate(
            [
                ref[pl.ds(pl.multiple_of(place(e, c, b) * block, block), block), :]
                for b in range(4)
            ],
            axis=0,
        )

    def first(e):
        left = left_rows(s.left, e, 1 - core)
        for i in range(count):
            if i < lows:
                s.sent[e, i] = product(left, i).astype(s.sent.dtype)
            else:
                s.high_sent[e, i - lows] = product(left, i)
        for copy in pair_copies(e):
            copy.start()

    def second(e):
        left = left_rows(s.left, e, core)
        for i in range(count):
            s.own[e, i] = product(left, i)

    each(0, 2, first)
    each(0, 2, second)

    at = (CHIPS - 1 - chip, chip)
    onward = (me - 2, me + 2)
    backward = (me + 2, me - 2)

    def part(j):
        return pl.ds(pl.multiple_of(j * chunk, chunk), chunk)

    def out_rows(e, c, j):
        start = place(e, c, j // per) * block + (j % per) * chunk
        return pl.ds(pl.multiple_of(start, chunk), chunk)

    def up_copy(e, j):
        return copy_to(
            s.up.at[e, :, part(j), :],
            s.down.at[e, :, part(j), :],
            s.up_send.at[e, j],
            s.up_recv.at[e, j],
            dp=onward[e],
        )

    def back_copy(e, j):
        view = gathered.at[:, out_rows(e, core, j), :]
        return copy_to(view, view, s.back_send.at[e, j], s.back_recv.at[e, j], dp=backward[e])

    def side_copy(e, j, c):
        view = gathered.at[:, out_rows(e, c, j), :]
        return copy_to(view, view, s.side_send.at[e, j], s.side_recv.at[e, j], dp=partner)

    def here(e, j):
        found = []
        for i in range(count):
            if i < lows:
                other = s.landed[e, i, part(j), :].astype(F32)
            else:
                other = s.high_landed[e, i - lows, part(j), :]
            found.append(s.own[e, i, part(j), :] + other)
        return found

    def send_up(e, j, values):
        for i in range(count):
            s.up[e, i, part(j), :] = values[i].astype(BF16)
        up_copy(e, j).start()

    for e in (0, 1):
        for copy in pair_copies(e):
            copy.wait_recv()

        @pl.when(at[e] == 0)
        def _():
            each(0, steps, lambda j: send_up(e, j, here(e, j)))

    def loop(t):
        for e in (0, 1):
            j = t - skew * (at[e] - 1)

            @pl.when((at[e] > 0) & (j >= 0) & (j < steps))
            def _():
                up_copy(e, j).wait_recv()
                total = [
                    value + s.down[e, i, part(j), :].astype(F32)
                    for i, value in enumerate(here(e, j))
                ]

                @pl.when(at[e] < CHIPS - 1)
                def _():
                    send_up(e, j, total)

                @pl.when(at[e] == CHIPS - 1)
                def _():
                    finish(total, part(j), out_rows(e, core, j))
                    back_copy(e, j).start()
                    side_copy(e, j, core).start()

        for e in (0, 1):
            j = t - skew * (2 * CHIPS - 3 - at[e])

            @pl.when((at[e] < CHIPS - 1) & (j >= 0) & (j < steps))
            def _():
                back_copy(e, j).wait_recv()

                @pl.when(at[e] > 0)
                def _():
                    back_copy(e, j).start()

                side_copy(e, j, core).start()

        if arrived is not None:
            for e in (0, 1):
                j = t - skew * (2 * CHIPS - 3 - at[e])

                @pl.when((j >= 0) & (j < steps) & (j % per == per - 1))
                def _():
                    arrived(place(e, core, j // per))

                k = j - 1

                @pl.when((k >= 0) & (k < steps) & (k % per == per - 1))
                def _():
                    each(k - (per - 1), k + 1, lambda i: side_copy(e, i, 1 - core).wait_recv())
                    arrived(place(e, 1 - core, k // per))

    each(0, steps + skew * (2 * CHIPS - 3) + (0 if arrived is None else 1), loop)

    def close(j):
        for e in (0, 1):
            if arrived is None:
                side_copy(e, j, 1 - core).wait_recv()
            side_copy(e, j, core).wait_send()

            @pl.when(at[e] < CHIPS - 1)
            def _():
                up_copy(e, j).wait_send()

            @pl.when(at[e] > 0)
            def _():
                back_copy(e, j).wait_send()

    def finally_():
        each(0, steps, close)
        for e in (0, 1):
            for copy in pair_copies(e):
                copy.wait_send()

    return finally_


def turned(rows_of):
    fill = jnp.zeros((LANES - len(rows_of), LANES), F32)
    return jnp.concatenate([*rows_of, fill], axis=0).T


def advantages(s, groups, members, count):
    lengths, prompts, rewards = (
        jnp.concatenate([s.meta[g, i : i + 1, :] for g in range(groups)], axis=0) for i in range(3)
    )
    before = lax.broadcasted_iota(jnp.int32, (LANES, LANES), 0) <= lax.broadcasted_iota(
        jnp.int32, (LANES, LANES), 1
    )
    ends = jnp.dot(
        lengths.astype(BF16),
        jnp.where(before, 1.0, 0.0).astype(BF16),
        preferred_element_type=F32,
    )
    starts = ends - lengths
    gaps = jnp.concatenate([s.gaps[f, 0:1, :] for f in range(members)], axis=0)
    first = lax.broadcasted_iota(jnp.int32, (members, LANES), 0).astype(F32) * count
    lane = lax.broadcasted_iota(jnp.int32, (members, LANES), 1)

    def inside(g, i):
        position = first + i
        return (position >= starts[g : g + 1, :]) & (position < ends[g : g + 1, :])

    sums = []
    for g in range(groups):
        found = jnp.zeros((members, LANES), F32)
        for i in range(count):
            column = g * count + i
            found += jnp.where(inside(g, i), gaps[:, column : column + 1], 0.0)
        sums.append(jnp.sum(found, axis=0, keepdims=True))
    scores = rewards - KL_WEIGHT * jnp.concatenate(sums, axis=0)
    others = -scores
    for prompt in range(s.lengths.shape[1] // K):
        same = prompts == prompt
        total = jnp.sum(jnp.where(same, scores, 0.0), axis=1, keepdims=True)
        others += jnp.where(same, total, 0.0)
    advantage = scores - others / (K - 1)
    weights = jnp.zeros((members, LANES), F32)
    for g in range(groups):
        for i in range(count):
            mine = jnp.where(inside(g, i), advantage[g : g + 1, :], 0.0)
            weights = jnp.where(
                lane == g * count + i, jnp.sum(mine, axis=1, keepdims=True), weights
            )
    return advantage, weights


def logits_phase(s, groups, members, me, member):
    plane, half = member // 2, member % 2
    mate = member + 1 - 2 * half
    rows, width = s.states.shape
    pair = 2 * rows

    def share(other):
        return copy_to(
            s.l_sent.at[other],
            s.l_landed.at[plane],
            s.l_send.at[other],
            s.l_recv.at[plane],
            fsdp=other * 2 + half,
        )

    def project(other):
        out = [
            jnp.dot(
                s.hidden[m, pl.ds(pl.multiple_of(other * pair, pair), pair), :],
                right[...],
                preferred_element_type=F32,
            )
            for m, right in enumerate((s.ref_down, s.pol_down))
        ]

        @pl.when(other == plane)
        def _():
            for m in (0, 1):
                s.total[m] = out[m]

        @pl.when(other != plane)
        def _():
            for m in (0, 1):
                s.l_sent[other, m] = out[m].astype(BF16)
            share(other).start()

    def rest():
        def add(step):
            source = lax.rem(plane + PLANE - step, PLANE)
            copy_to(
                s.l_sent.at[source],
                s.l_landed.at[source],
                s.l_send.at[source],
                s.l_recv.at[source],
                fsdp=source * 2 + half,
            ).wait_recv()
            s.total[...] += s.l_landed[source].astype(F32)

        each(1, PLANE, add)
        theirs = pl.ds(pl.multiple_of((1 - half) * rows, rows), rows)
        mine = pl.ds(pl.multiple_of(half * rows, rows), rows)
        s.mate_ref[...] = s.total[0, theirs, :].astype(BF16)
        s.mate_pol[...] = s.total[1, theirs, :]
        mate_copies = (
            copy_to(s.mate_ref, s.mate_ref_in, s.h_send.at[0], s.h_recv.at[0], fsdp=mate),
            copy_to(s.mate_pol, s.mate_pol_in, s.h_send.at[1], s.h_recv.at[1], fsdp=mate),
        )
        for copy in mate_copies:
            copy.start()
        s.pol_hidden[...] = s.hidden[1]
        for copy in mate_copies:
            copy.wait_recv()
        logits = [
            s.states[...] + s.total[0, mine, :] + s.mate_ref_in[...].astype(F32),
            s.states[...] + s.total[1, mine, :] + s.mate_pol_in[...],
        ]
        columns = lax.broadcasted_iota(jnp.int32, (rows, width), 1) + me * width
        picked = columns.astype(F32) == s.id_rows[:, 0:1]
        lane = lax.broadcasted_iota(jnp.int32, (rows, LANES), 1)
        tile = jnp.zeros((rows, LANES), F32)
        for m in (0, 1):
            peak = jnp.max(logits[m], axis=1, keepdims=True)
            summed = jnp.sum(jnp.exp(logits[m] - peak), axis=1, keepdims=True)
            pick = jnp.sum(jnp.where(picked, logits[m], 0.0), axis=1, keepdims=True)
            for i, value in enumerate((peak, summed, pick)):
                tile = jnp.where(lane == 3 * m + i, value, tile)
        full = jnp.concatenate([tile, jnp.zeros((LANES - rows, LANES), F32)], axis=0)
        s.stats[...] = full.T[0:8, :]
        start, wait, done = row_exchange(
            me, groups, lambda p: s.stats, lambda g: s.stats_all.at[g], s.s_send, s.s_recv
        )
        start()
        s.stats_all[me] = s.stats[...]
        wait()
        real = lax.broadcasted_iota(jnp.int32, (1, LANES), 1) < rows
        log_totals, logprobs = [], []
        for m in (0, 1):
            peaks = [s.stats_all[g, 3 * m : 3 * m + 1, :] for g in range(groups)]
            peak = functools.reduce(jnp.maximum, peaks)
            summed = sum(
                s.stats_all[g, 3 * m + 1 : 3 * m + 2, :] * jnp.exp(peaks[g] - peak)
                for g in range(groups)
            )
            pick = sum(s.stats_all[g, 3 * m + 2 : 3 * m + 3, :] for g in range(groups))
            log_total = peak + jnp.log(jnp.where(real, summed, 1.0))
            log_totals.append(log_total)
            logprobs.append(pick - log_total)
        s.gaps[member] = jnp.broadcast_to(logprobs[1] - logprobs[0], (8, LANES))
        log_total = turned([log_totals[1]])[0:rows, 0:1]
        grad = jnp.where(picked, 1.0, 0.0) - jnp.exp(logits[1] - log_total)
        s.raw[pl.ds(pl.multiple_of(member * rows, rows), rows), :] = grad.astype(BF16)
        views = (
            lambda b: s.gaps.at[b],
            lambda b: s.raw.at[pl.ds(pl.multiple_of(b * rows, rows), rows), :],
        )
        plane_gather(member, views, s.g_mate_send, s.g_mate_recv, s.g_send, s.g_recv)
        done()
        for copy in mate_copies:
            copy.wait_send()
        each(1, PLANE, lambda step: share(lax.rem(plane + step, PLANE)).wait_send())
        advantage, weights = advantages(s, groups, members, rows // groups)
        s.advantage_rows[...] = advantage
        s.advantage[...] = s.advantage_rows[pl.ds(me, 1), 0 : s.advantage.shape[1]]
        fill = jnp.zeros((LANES - members, LANES), F32)
        turned_weights = jnp.concatenate([weights, fill], axis=0).T
        for f in range(members):
            at = slice(f * rows, (f + 1) * rows)
            s.grads[at, :] = (
                -turned_weights[0:rows, f : f + 1] * s.raw[at, :].astype(F32)
            ).astype(BF16)

    return project, rest


def step_kernel(names, groups, members, forward_steps, backward_steps, skew, *refs):
    s = SimpleNamespace(**dict(zip(names, refs)))
    me, member = lax.axis_index("dp"), lax.axis_index("fsdp")
    plane = member // 2
    greet_all(me, groups, member)
    norm_phase(s, groups, me, member)
    project, rest = logits_phase(s, groups, members, me, member)

    def parts(prefix, left):
        found = {
            name: getattr(s, prefix + name, None)
            for name in RUN_NAMES + ("high_sent", "high_landed", "high_send", "high_recv")
        }
        return SimpleNamespace(left=left, **found)

    weights = (s.ref_gate, s.ref_up, s.pol_gate, s.pol_up)

    def units(left, right):
        return lax.dot_general(
            left, right, (((1,), (1,)), ((), ())), preferred_element_type=F32
        )

    def activate(total, rows, out_rows):
        for m in (0, 1):
            gate, up_value = total[2 * m], total[2 * m + 1]
            s.hidden[m, out_rows, :] = (gate * jax.nn.sigmoid(gate) * up_value).astype(BF16)
        s.pre[0, rows, :] = total[2]
        s.pre[1, rows, :] = total[3]

    close_forward = run_reduce(
        forward_steps,
        skew,
        me,
        plane,
        lambda left, i: units(left, weights[i][...]),
        activate,
        s.hidden,
        parts("f_", s.normed),
        project,
    )
    rest()
    close_forward()

    def differentiate(total, rows, out_rows):
        grad_hidden, gate, up_value = total[0], s.pre[0, rows, :], s.pre[1, rows, :]
        sigmoid = jax.nn.sigmoid(gate)
        s.gates[0, out_rows, :] = (
            grad_hidden * up_value * sigmoid * (1.0 + gate * (1.0 - sigmoid))
        ).astype(BF16)
        s.gates[1, out_rows, :] = (grad_hidden * gate * sigmoid).astype(BF16)

    run_reduce(
        backward_steps,
        skew,
        me,
        plane,
        lambda left, i: units(left, s.pol_down[...]),
        differentiate,
        s.gates,
        parts("b_", s.grads),
    )()


RUN_NAMES = (
    "own",
    "sent",
    "landed",
    "up",
    "down",
    "pair_send",
    "pair_recv",
    "up_send",
    "up_recv",
    "back_send",
    "back_recv",
    "side_send",
    "side_recv",
)


def run_scratch(prefix, count, lows, quarter, units, steps):
    wide = lambda n, kind: pltpu.VMEM((2, n, quarter, units), kind)
    shapes = [wide(count, F32), wide(lows, BF16), wide(lows, BF16)]
    shapes += [wide(count, BF16)] * 2 + [DMA((2,))] * 2 + [DMA((2, steps))] * 6
    found = {prefix + name: shape for name, shape in zip(RUN_NAMES, shapes)}
    if lows < count:
        found[prefix + "high_sent"] = found[prefix + "high_landed"] = wide(count - lows, F32)
        found[prefix + "high_send"] = found[prefix + "high_recv"] = DMA((2,))
    return found


FORWARD_STEPS, BACKWARD_STEPS, SKEW = 16, 8, 3


def one_step(inputs, groups, members):
    count, width = inputs["rows"].shape
    samples = inputs["lengths"].shape[1]
    units = inputs["ref_gate"].shape[0]
    block, rows = width // groups, groups * count
    tokens = members * rows
    quarter = tokens // 4
    shape = jax.ShapeDtypeStruct
    outputs = {
        "normed": shape((tokens, block), BF16),
        "gates": shape((2, tokens, units), BF16),
        "pol_hidden": shape((tokens, units), BF16),
        "grads": shape((tokens, block), BF16),
        "advantage": shape((1, samples), F32),
    }
    gather = lambda n: [DMA((n,)), DMA((n,)), DMA((n, 2, PLANE)), DMA((n, 2, PLANE))]
    scratch = {
        "row_sent": pltpu.VMEM((groups, count, block), BF16),
        "row_landed": pltpu.VMEM((groups, count, block), BF16),
        "meta_sent": pltpu.VMEM((8, LANES), F32),
        "meta": pltpu.VMEM((groups, 8, LANES), F32),
        "states": pltpu.VMEM((rows, block), F32),
        "scaled": pltpu.VMEM((rows, block), F32),
        "id_rows": pltpu.VMEM((rows, LANES), F32),
        **{name: DMA((groups,)) for name in ("r_send", "r_recv", "m_send", "m_recv")},
        **dict(zip(("n_mate_send", "n_mate_recv", "n_send", "n_recv"), gather(1))),
        **run_scratch("f_", 4, 2, quarter, units, FORWARD_STEPS),
        "hidden": pltpu.VMEM((2, tokens, units), BF16),
        "pre": pltpu.VMEM((2, quarter, units), F32),
        "l_sent": pltpu.VMEM((PLANE, 2, 2 * rows, block), BF16),
        "l_landed": pltpu.VMEM((PLANE, 2, 2 * rows, block), BF16),
        "l_send": DMA((PLANE,)),
        "l_recv": DMA((PLANE,)),
        "total": pltpu.VMEM((2, 2 * rows, block), F32),
        "mate_ref": pltpu.VMEM((rows, block), BF16),
        "mate_ref_in": pltpu.VMEM((rows, block), BF16),
        "mate_pol": pltpu.VMEM((rows, block), F32),
        "mate_pol_in": pltpu.VMEM((rows, block), F32),
        "h_send": DMA((2,)),
        "h_recv": DMA((2,)),
        "stats": pltpu.VMEM((8, LANES), F32),
        "stats_all": pltpu.VMEM((groups, 8, LANES), F32),
        "s_send": DMA((groups,)),
        "s_recv": DMA((groups,)),
        "raw": pltpu.VMEM((tokens, block), BF16),
        "gaps": pltpu.VMEM((members, 8, LANES), F32),
        "advantage_rows": pltpu.VMEM((groups, LANES), F32),
        **dict(zip(("g_mate_send", "g_mate_recv", "g_send", "g_recv"), gather(2))),
        **run_scratch("b_", 1, 1, quarter, units, BACKWARD_STEPS),
    }
    names = (*inputs, *outputs, *scratch)
    results = pl.pallas_call(
        functools.partial(
            step_kernel, names, groups, members, FORWARD_STEPS, BACKWARD_STEPS, SKEW
        ),
        out_shape=tuple(outputs.values()),
        in_specs=[VMEM] * len(inputs),
        out_specs=(VMEM,) * len(outputs),
        scratch_shapes=list(scratch.values()),
        compiler_params=pltpu.CompilerParams(collective_id=0, has_side_effects=True),
        name="one_step",
    )(*inputs.values())
    return dict(zip(outputs, results))


def local(
    hidden_states,
    token_ids,
    norm_gain,
    ref_gate_w,
    ref_up_w,
    ref_down_w,
    pol_gate_w,
    pol_up_w,
    pol_down_w,
    sample_lengths,
    prompt_index,
    rewards,
):
    found = one_step(
        {
            "rows": hidden_states,
            "gain": norm_gain.reshape(1, -1),
            "lengths": sample_lengths,
            "prompts": prompt_index,
            "rewards": rewards,
            "ids": token_ids.reshape(1, -1),
            "ref_gate": ref_gate_w.T,
            "ref_up": ref_up_w.T,
            "pol_gate": pol_gate_w.T,
            "pol_up": pol_up_w.T,
            "ref_down": ref_down_w,
            "pol_down": pol_down_w,
        },
        lax.axis_size("dp"),
        lax.axis_size("fsdp"),
    )

    def outer(left, right):
        return lax.dot_general(
            left, right, (((0,), (0,)), ((), ())), preferred_element_type=F32
        )

    return (
        outer(found["normed"], found["gates"][0]),
        outer(found["normed"], found["gates"][1]),
        outer(found["pol_hidden"], found["grads"]),
        found["advantage"],
    )


def solution(mesh):
    return jax.shard_map(
        local,
        mesh=mesh,
        in_specs=(
            P(("dp", "fsdp"), None),
            P(("dp", "fsdp")),
            P(),
            P("dp", "fsdp"),
            P("dp", "fsdp"),
            P("fsdp", "dp"),
            P("dp", "fsdp"),
            P("dp", "fsdp"),
            P("fsdp", "dp"),
            P("dp", None),
            P("dp", None),
            P("dp", None),
        ),
        out_specs=(P("dp", "fsdp"), P("dp", "fsdp"), P("fsdp", "dp"), P("dp", None)),
        check_vma=False,
    )
```
